32 devices in a mesh: seq: 8 (over y, x, core), head: 4 (over z).
Axes of the slice: x: 2, y: 2, z: 4, core: 2. Of those that a mesh axis runs over, the one named last changes fastest.
Arguments:
- latent_cache: bfloat16 [2, 16384, 576], P(None, 'seq'), may hold values from -8 to 8
- draft_latent: bfloat16 [2, 64, 576], P(None, 'seq'), may hold values from -9 to 9
- query_nope: bfloat16 [2, 64, 128, 128], P(None, None, 'head'), may hold values from -6 to 6
- query_rope: bfloat16 [2, 64, 128, 64], P(None, None, 'head'), may hold values from -8 to 8
- parents: int32 [2, 64], replicated, may hold values from -1 to 62, as said below
- lengths: int32 [2], replicated, may hold values from 8192 to 16384
- key_weight: bfloat16 [128, 128, 512], P('head'), may hold values from -0.25 to 0.25
- value_weight: bfloat16 [128, 512, 128], P('head'), may hold values from -0.25 to 0.25
- out_weight: bfloat16 [16384, 7168], P('head', 'seq'), may hold values from -0.046875 to 0.046875
- residual: bfloat16 [2, 64, 7168], P(None, None, 'seq'), may hold values from -40 to 40
- norm_gain: bfloat16 [7168], P('seq'), may hold values from 0.5 to 1.5
- vocab_weight: bfloat16 [7168, 8192], P('seq', 'head'), may hold values from -0.21875 to 0.21875
Outputs:
- logits: bfloat16 [2, 64, 8192], P(None, None, ('head', 'seq'))
The draws below stay inside these ranges and needn't reach their ends.
Inputs may be any that keep to these rules, and one draw needn't show every extreme that they name: `parents`: token 0 is the root of each tree with parent -1; every other token's parent is an earlier token; the last token's parent is the token just before it.
All inputs are finite; a program needn't handle non-finite values.
Results may differ from the reference program's by a relative error of at most 0.02.
Values may be sent and summed in bfloat16 or wider, within the bound.
No kernel may reach another device: no remote copies, remote signals or barrier semaphores. Data moves between devices by JAX's collectives and lax.ppermute only.
A program may use at most 128 MiB of HBM per device.

```python
import math
import jax
import jax.numpy as jnp
from jax import lax

HEADS = 128
NOPE = 128
ROPE = 64
LAT = 512
VH = 128
D = 7168
REQUESTS = 2
DRAFT = 64
CTX = 16384
VOCAB = 8192


def draw_latent_cache(key, part):
    baseline = jnp.clip(jax.random.normal(jax.random.fold_in(key, 1), (REQUESTS, CTX, LAT + ROPE)), -6.0, 6.0)
    return baseline.astype(jnp.bfloat16)


def draw_query_rope(key, part):
    baseline = jnp.clip(jax.random.normal(jax.random.fold_in(key, 2), (REQUESTS, DRAFT, HEADS, ROPE)), -6.0, 6.0)
    return baseline.astype(jnp.bfloat16)


def draw_parents(key, part):
    indices = jnp.arange(DRAFT, dtype=jnp.int32)
    upper = jnp.maximum(indices, 1)[None, :]
    picked = jax.random.randint(jax.random.fold_in(key, 3), (REQUESTS, DRAFT), 0, upper)
    picked = jnp.where(indices[None, :] == DRAFT - 1, DRAFT - 2, picked)
    return jnp.where(indices[None, :] == 0, -1, picked).astype(jnp.int32)


def draw_residual(key, part):
    key_rows, key_cols, key_noise = jax.random.split(jax.random.fold_in(key, 4), 3)
    row_scale = jnp.exp(jax.random.uniform(key_rows, (REQUESTS, DRAFT, 1), minval=math.log(0.03), maxval=math.log(0.3)))
    rising = 3.0 ** (jnp.arange(D, dtype=jnp.float32) / D)
    col_scale = jnp.exp(jax.random.uniform(key_cols, (D,), minval=math.log(0.5), maxval=math.log(5.0))) * rising
    noise = jnp.clip(jax.random.normal(key_noise, (REQUESTS, DRAFT, D)), -4.0, 4.0)
    return (noise * row_scale * col_scale).astype(jnp.bfloat16)


def block_levels(key, extent, cuts, smallest, top_value):
    factor_of = 1.0
    for dim, blocks in cuts:
        heights = jax.random.uniform(jax.random.fold_in(jax.random.fold_in(key, 6), dim), (blocks,), jnp.float32, smallest / len(cuts), top_value / len(cuts))
        factor_of = factor_of * jnp.repeat(jnp.exp(heights), extent[dim] // blocks).reshape((-1,) + (1,) * (len(extent) - 1 - dim))
    return factor_of


def normal_values(key, extent, scale, limit, cuts=(), kind=jnp.bfloat16):
    result = jax.random.normal(key, extent, jnp.float32) * scale
    if len(cuts) > 0:
        result = block_levels(key, extent, cuts, -0.22, 0.18) * result
    return jnp.clip(result, min=-limit, max=limit).astype(kind)


def setup_inputs(seed: int = 0) -> dict:
    key_list = jax.random.split(jax.random.key(seed), 13)
    latent_cache = draw_latent_cache(jax.random.fold_in(key_list[12], 71), 0)
    draft_latent = normal_values(key_list[1], (REQUESTS, DRAFT, LAT + ROPE), 3.0, 9.0, ((1, 8),))
    query_nope = normal_values(key_list[2], (REQUESTS, DRAFT, HEADS, NOPE), 1.0, 6.0, ((2, 4),))
    query_rope = draw_query_rope(jax.random.fold_in(key_list[12], 71), 0)
    parents = draw_parents(jax.random.fold_in(key_list[12], 71), 0)
    lengths = jax.random.randint(key_list[5], (REQUESTS,), CTX // 2, CTX + 1).astype(jnp.int32)
    key_weight = normal_values(key_list[6], (HEADS, NOPE, LAT), LAT ** -0.5, 0.25, ((0, 4),))
    value_weight = normal_values(key_list[7], (HEADS, LAT, VH), LAT ** -0.5, 0.25, ((0, 4),))
    out_weight = normal_values(key_list[8], (HEADS * VH, D), (HEADS * VH) ** -0.5, 0.046875, ((0, 4), (1, 8)))
    residual = draw_residual(jax.random.fold_in(key_list[12], 71), 0)
    norm_gain = jnp.clip(1.0 + 0.1 * jax.random.normal(key_list[10], (D,), jnp.float32), 0.5, 1.5).astype(jnp.bfloat16)
    vocab_weight = normal_values(key_list[11], (D, VOCAB), (D // 9) ** -0.5, 0.21875, ((0, 8), (1, 4)))
    return dict(latent_cache=latent_cache, draft_latent=draft_latent, query_nope=query_nope, query_rope=query_rope, parents=parents, lengths=lengths, key_weight=key_weight, value_weight=value_weight, out_weight=out_weight, residual=residual, norm_gain=norm_gain, vocab_weight=vocab_weight)


NEGATIVE = -1e+30
EPSILON = 1e-06

def ancestry_of(parents):
    token_count = parents.shape[1]
    indices = jnp.arange(token_count, dtype=jnp.int32)
    linked = (parents[:, :, None] == indices[None, None, :]) | (indices[:, None] == indices[None, :])[None]
    reachable = linked.astype(jnp.float32)
    for repeat in range(max(1, (token_count - 1).bit_length())):
        product = jnp.einsum('bij,bjk->bik', reachable, reachable, precision=lax.Precision.HIGHEST)
        reachable = jnp.where(product > 0.5, 1.0, 0.0).astype(jnp.float32)
    return reachable

def reference(latent_cache, draft_latent, query_nope, query_rope, parents, lengths, key_weight, value_weight, out_weight, residual, norm_gain, vocab_weight):
    scaling = 1.0 / math.sqrt(NOPE + ROPE)
    absorbed = jnp.einsum('bthn,hnl->bthl', query_nope.astype(jnp.float32), key_weight.astype(jnp.float32)).astype(jnp.bfloat16)
    queries = jnp.concatenate([absorbed, query_rope], axis=-1)
    ancestry = ancestry_of(parents)
    live = jnp.arange(CTX, dtype=jnp.int32)[None, :] < lengths[:, None]
    cache_keys = latent_cache.astype(jnp.float32)
    draft_keys = draft_latent.astype(jnp.float32)
    cache_values = cache_keys[:, :, :LAT]
    draft_values = draft_keys[:, :, :LAT]

    def one_head(inputs):
        head_query, head_value = inputs
        query_full = head_query.astype(jnp.float32)
        cache_scores = jnp.einsum('btc,bkc->btk', query_full, cache_keys) * scaling
        cache_scores = jnp.where(live[:, None, :], cache_scores, NEGATIVE)
        draft_scores = jnp.einsum('btc,bkc->btk', query_full, draft_keys) * scaling
        draft_scores = jnp.where(ancestry > 0.5, draft_scores, NEGATIVE)
        largest = jnp.maximum(lax.optimization_barrier(jnp.max(cache_scores, -1)), lax.optimization_barrier(jnp.max(draft_scores, -1)))
        cache_weights = jnp.where(live[:, None, :], jnp.exp(cache_scores - largest[..., None]), 0.0)
        draft_weights = jnp.where(ancestry > 0.5, jnp.exp(draft_scores - largest[..., None]), 0.0)
        total = lax.optimization_barrier(jnp.sum(cache_weights, -1)) + lax.optimization_barrier(jnp.sum(draft_weights, -1))
        mixed = jnp.einsum('btk,bkl->btl', cache_weights.astype(jnp.bfloat16).astype(jnp.float32), cache_values)
        mixed = mixed + jnp.einsum('btk,bkl->btl', draft_weights.astype(jnp.bfloat16).astype(jnp.float32), draft_values)
        latent_out = (mixed / total[..., None]).astype(jnp.bfloat16)
        return jnp.einsum('btl,lv->btv', latent_out.astype(jnp.float32), head_value.astype(jnp.float32)).astype(jnp.bfloat16)
    head_out = lax.map(one_head, (jnp.moveaxis(queries, 2, 0), value_weight))
    head_out = jnp.moveaxis(head_out, 0, 2).reshape(REQUESTS * DRAFT, HEADS * VH)
    attention = jnp.dot(head_out, out_weight, preferred_element_type=jnp.float32).reshape(REQUESTS, DRAFT, D)
    hidden = residual.astype(jnp.float32) + attention
    mean_square = lax.optimization_barrier(jnp.mean(hidden * hidden, -1, keepdims=True))
    normed = (hidden * lax.rsqrt(mean_square + EPSILON) * norm_gain.astype(jnp.float32)).astype(jnp.bfloat16)
    logits = jnp.dot(normed.reshape(REQUESTS * DRAFT, D), vocab_weight, preferred_element_type=jnp.float32)
    return logits.reshape(REQUESTS, DRAFT, VOCAB).astype(jnp.bfloat16)
```

```python
import functools
import math

import jax
import jax.numpy as jnp
from jax import lax
from jax.experimental import pallas as pl
from jax.experimental.pallas import tpu as pltpu
from jax.sharding import PartitionSpec as P


NEGATIVE = -1e30
EPSILON = 1e-06
LANES = 128
F32 = jnp.float32
BF16 = jnp.bfloat16
VMEM = pltpu.CompilerParams(vmem_limit_bytes=56 * 1024 * 1024)


def dot(a, b):
    return jnp.dot(a, b, preferred_element_type=F32)


def dot_t(a, b):
    return lax.dot_general(a, b, (((1,), (1,)), ((), ())), preferred_element_type=F32)


def eye_mask(rows):
    return lax.broadcasted_iota(jnp.int32, (rows, LANES), 0) == lax.broadcasted_iota(
        jnp.int32, (rows, LANES), 1
    )


def to_row(column, mask):
    return jnp.sum(jnp.where(mask, column, 0.0), axis=0, keepdims=True)


def to_column(row, mask):
    return jnp.sum(jnp.where(mask, row, 0.0), axis=1, keepdims=True)


def split3(x):
    hi = x.astype(BF16).astype(F32)
    mid = (x - hi).astype(BF16).astype(F32)
    lo = x - hi - mid
    return hi, mid, lo


def pad_rows(x, rows):
    if x.shape[0] == rows:
        return x
    return jnp.concatenate([x, jnp.zeros((rows - x.shape[0], x.shape[1]), x.dtype)], axis=0)


def attend_kernel(
    seat_ref, len_ref, link_ref, draft_ref, qn_hbm, qr_hbm, kw_hbm, vw_hbm, cache_hbm,
    o_ref, lse_ref,
    qn, qr, qnf, qrf, kw, vw, keys, q0, q1, s0, s1, p0, p1, tree, sems,
    *, group, drafted, draft_local, scaling,
):
    requests, width, cache_local = cache_hbm.shape
    heads, latent, _ = vw_hbm.shape
    rows = requests * drafted
    steps = heads // group
    q_refs, s_refs, p_refs = (q0, q1), (s0, s1), (p0, p1)
    chunk = 256
    copies = [
        pltpu.make_async_copy(qn_hbm, qn, sems.at[0]),
        pltpu.make_async_copy(kw_hbm, kw, sems.at[1]),
        pltpu.make_async_copy(qr_hbm, qr, sems.at[2]),
        pltpu.make_async_copy(cache_hbm.at[0], keys.at[0, :, pl.ds(0, cache_local)], sems.at[3]),
        pltpu.make_async_copy(cache_hbm.at[1], keys.at[1, :, pl.ds(0, cache_local)], sems.at[4]),
        pltpu.make_async_copy(vw_hbm, vw, sems.at[5]),
    ]
    for copy in copies:
        copy.start()
    seat = seat_ref[0]
    scale2 = scaling * math.log2(math.e)

    lane = lax.broadcasted_iota(jnp.int32, (rows, rows), 1)
    sub = lax.broadcasted_iota(jnp.int32, (rows, rows), 0)
    reach = jnp.where((link_ref[...] == lane) | (lane == sub), 1.0, 0.0).astype(BF16)
    for _ in range(max(1, (drafted - 1).bit_length())):
        reach = jnp.where(dot(reach, reach) > 0.5, 1.0, 0.0).astype(BF16)
    pick_sub = lax.broadcasted_iota(jnp.int32, (rows, LANES), 0)
    pick_lane = lax.broadcasted_iota(jnp.int32, (rows, LANES), 1)
    for b in range(requests):
        pick = (pick_sub == b * drafted + seat * draft_local + pick_lane) & (
            pick_lane < draft_local
        )
        own = dot(reach, jnp.where(pick, 1.0, 0.0).astype(BF16))
        tree[b] = own[b * drafted : (b + 1) * drafted]
        keys[b, :, cache_local:] = draft_ref[b]

    mask = eye_mask(drafted)

    def absorb(g):
        for i in range(group):
            h = g * group + i
            at = pl.ds(h, rows, stride=heads)
            a = dot(qnf[at, :].astype(BF16), kw[h]).astype(BF16)
            r = qrf[at, :].astype(BF16)
            for b in range(requests):
                src = slice(b * drafted, (b + 1) * drafted)
                dst = slice(i * drafted, (i + 1) * drafted)
                q_refs[b][dst, :latent] = a[src]
                q_refs[b][dst, latent:] = r[src]

    def score_pieces(b):
        live = len_ref[b] - seat * cache_local

        def cached(n):
            s = dot(q_refs[b][...], keys[b, :, n : n + chunk])
            at = lax.broadcasted_iota(jnp.int32, (1, chunk), 1) + n
            s_refs[b][:, n : n + chunk] = s * scale2 + jnp.where(at < live, 0.0, NEGATIVE)

        def drafts():
            s = dot(q_refs[b][...], keys[b, :, cache_local:])
            for i in range(group):
                at = slice(i * drafted, (i + 1) * drafted)
                s_refs[b][at, cache_local:] = jnp.where(tree[b] > 0.5, s[at] * scale2, NEGATIVE)

        pieces = [functools.partial(cached, n) for n in range(0, cache_local, chunk)]
        return pieces + [drafts]

    def soft_pieces(b, stats):
        total_keys = cache_local + LANES
        s_ref, p_ref = s_refs[b], p_refs[b]

        def piece(i):
            at = slice(i * drafted, (i + 1) * drafted)
            top = s_ref[at, 0:LANES]
            for n in range(LANES, total_keys, LANES):
                top = jnp.maximum(top, s_ref[at, n : n + LANES])
            top = jnp.max(top, axis=1, keepdims=True)
            total = None
            for n in range(0, total_keys, LANES):
                p = jnp.exp2(s_ref[at, n : n + LANES] - top)
                p_ref[at, n : n + LANES] = p.astype(BF16)
                total = p if total is None else total + p
            total = jnp.sum(total, axis=1, keepdims=True)
            stats.append((total, top + jnp.log2(total)))

        return [functools.partial(piece, i) for i in range(group)]

    def finish(g, b, stats):
        mixed = dot_t(p_refs[b][...], keys[b, :latent, :])
        for i in range(group):
            h = g * group + i
            total, lse = stats[i]
            m = (mixed[i * drafted : (i + 1) * drafted] / total).astype(BF16)
            o_ref[b, h] = dot(m, vw[h]).astype(BF16)
            lse_ref[b, pl.ds(h, 1), :] = to_row(lse, mask)

    def interleave(b_next, g, b):
        stats = []
        first = score_pieces(b_next) if b_next is not None else []
        second = soft_pieces(b, stats)
        count = max(len(first), len(second))
        done = 0
        for j in range(count):
            if j < len(first):
                first[j]()
            while done < len(second) and done * max(len(first), 1) <= j * len(second):
                second[done]()
                done += 1
        while done < len(second):
            second[done]()
            done += 1
        finish(g, b, stats)

    copies[0].wait()
    copies[2].wait()
    qnf[...] = qn[...].astype(F32)
    qrf[...] = qr[...].astype(F32)
    copies[1].wait()
    absorb(0)
    copies[3].wait()
    for piece in score_pieces(0):
        piece()
    copies[4].wait()
    copies[5].wait()

    def step(g, carry):
        interleave(1, g, 0)
        absorb(g + 1)
        interleave(0, g, 1)
        return carry

    if steps > 1:
        lax.fori_loop(0, steps - 1, step, 0)
    interleave(1, steps - 1, 0)
    interleave(None, steps - 1, 1)


def attend(seat, lengths, link, draft, qn, qr, kw, vw, cache, drafted, draft_local, scaling):
    requests, width, cache_local = cache.shape
    heads = kw.shape[0]
    latent, value = vw.shape[1], vw.shape[2]
    group = math.gcd(heads, 4)
    block = group * drafted
    keys = cache_local + LANES
    hbm = pl.BlockSpec(memory_space=pl.ANY)
    smem = pl.BlockSpec(memory_space=pltpu.SMEM)
    vmem = pl.BlockSpec(memory_space=pltpu.VMEM)
    return pl.pallas_call(
        functools.partial(
            attend_kernel, group=group, drafted=drafted, draft_local=draft_local, scaling=scaling
        ),
        out_shape=(
            jax.ShapeDtypeStruct((requests, heads, drafted, value), BF16),
            jax.ShapeDtypeStruct((requests, heads, LANES), F32),
        ),
        in_specs=[smem, smem, vmem, vmem, hbm, hbm, hbm, hbm, hbm],
        out_specs=(vmem, vmem),
        scratch_shapes=[
            pltpu.VMEM(qn.shape, BF16),
            pltpu.VMEM(qr.shape, BF16),
            pltpu.VMEM(qn.shape, F32),
            pltpu.VMEM(qr.shape, F32),
            pltpu.VMEM(kw.shape, BF16),
            pltpu.VMEM(vw.shape, BF16),
            pltpu.VMEM((requests, width, keys), BF16),
            pltpu.VMEM((block, width), BF16),
            pltpu.VMEM((block, width), BF16),
            pltpu.VMEM((block, keys), F32),
            pltpu.VMEM((block, keys), F32),
            pltpu.VMEM((block, keys), BF16),
            pltpu.VMEM((block, keys), BF16),
            pltpu.VMEM((requests, drafted, LANES), F32),
            pltpu.SemaphoreType.DMA((6,)),
        ],
        compiler_params=VMEM,
        name="attend",
    )(seat, lengths, link, draft, qn, qr, kw, vw, cache)


def join_kernel(seat_ref, o_ref, lse_ref, po_ref, plse_ref, *outs, chips):
    seat = seat_ref[0]
    core, chip = seat % 2, seat // 2
    _, heads, drafted, value = o_ref.shape
    per = heads // chips
    mask = eye_mask(drafted)
    tail = max(8, per)
    for k in range(chips):
        at = (chip + k) % chips
        rows = []
        for j in range(per):
            h = at * per + j
            a = lse_ref[core, pl.ds(h, 1), :]
            b = plse_ref[pl.ds(h, 1), :]
            top = jnp.maximum(a, b)
            wa, wb = jnp.exp2(a - top), jnp.exp2(b - top)
            total = wa + wb
            rows.append(top + jnp.log2(total))
            ca, cb = to_column(wa / total, mask), to_column(wb / total, mask)
            mixed = o_ref[core, h].astype(F32) * ca + po_ref[h].astype(F32) * cb
            outs[k][j * drafted : (j + 1) * drafted, :] = mixed.astype(BF16)
        lse = pad_rows(jnp.concatenate(rows, axis=0) if per > 1 else rows[0], tail)
        hi, mid, lo = split3(lse)
        extra = jnp.concatenate([hi, mid, lo, jnp.zeros_like(lo)], axis=0)
        outs[k][per * drafted :, :] = extra.astype(BF16)


def join(seat, o, lse, other_o, other_lse, chips):
    _, heads, drafted, value = o.shape
    per = heads // chips
    shape = (per * drafted + 4 * max(8, per), value)
    smem = pl.BlockSpec(memory_space=pltpu.SMEM)
    vmem = pl.BlockSpec(memory_space=pltpu.VMEM)
    return pl.pallas_call(
        functools.partial(join_kernel, chips=chips),
        out_shape=[jax.ShapeDtypeStruct(shape, BF16)] * chips,
        in_specs=[smem] + [vmem] * 4,
        out_specs=[vmem] * chips,
        compiler_params=VMEM,
        name="join",
    )(seat, o, lse, other_o, other_lse)


def combine_kernel(*refs, per, drafted):
    blocks, out = refs[:-1], refs[-1]
    mask = eye_mask(drafted)
    tail = max(8, per)
    base = per * drafted
    lses = []
    for ref in blocks:
        extra = ref[base:, :].astype(F32)
        lses.append(extra[:tail] + extra[tail : 2 * tail] + extra[2 * tail : 3 * tail])
    top = functools.reduce(jnp.maximum, lses)
    weights = [jnp.exp2(x - top) for x in lses]
    total = functools.reduce(jnp.add, weights)
    weights = [w / total for w in weights]
    for j in range(per):
        at = slice(j * drafted, (j + 1) * drafted)
        acc = None
        for ref, w in zip(blocks, weights):
            term = ref[at, :].astype(F32) * to_column(w[j : j + 1], mask)
            acc = term if acc is None else acc + term
        out[at, :] = acc.astype(BF16)


def combine(blocks, per, drafted):
    vmem = pl.BlockSpec(memory_space=pltpu.VMEM)
    return pl.pallas_call(
        functools.partial(combine_kernel, per=per, drafted=drafted),
        out_shape=jax.ShapeDtypeStruct((per * drafted, blocks[0].shape[1]), BF16),
        in_specs=[vmem] * len(blocks),
        out_specs=vmem,
        compiler_params=VMEM,
        name="combine",
    )(*blocks)


def project_kernel(seat_ref, *refs, chips, per, drafted):
    mine, theirs = refs[:chips], refs[chips : 2 * chips]
    w_hbm, out, w, sems = refs[2 * chips :]
    seat = seat_ref[0]
    core, chip = seat % 2, seat // 2
    depth = w.shape[1]
    copies = []
    for k in range(chips):
        at = (chip - k + chips) % chips
        copies.append(
            pltpu.make_async_copy(
                w_hbm.at[pl.ds(pl.multiple_of(at * depth, depth), depth)], w.at[k], sems.at[k]
            )
        )
        copies[-1].start()
    acc = None
    for k in range(chips):
        sides = []
        for side in (mine[k], theirs[k]):
            parts = [side[j * drafted : (j + 1) * drafted, :] for j in range(per)]
            sides.append(jnp.concatenate(parts, axis=1) if per > 1 else parts[0])
        x = jnp.concatenate(sides, axis=0)
        copies[k].wait()
        term = dot(x, w[k])
        acc = term if acc is None else acc + term
    acc = acc.astype(BF16)
    out[core] = acc[:drafted]
    out[1 - core] = acc[drafted:]


def project(seat, mine, theirs, w, per, drafted):
    chips = len(mine)
    depth = w.shape[0] // chips
    smem = pl.BlockSpec(memory_space=pltpu.SMEM)
    vmem = pl.BlockSpec(memory_space=pltpu.VMEM)
    return pl.pallas_call(
        functools.partial(project_kernel, chips=chips, per=per, drafted=drafted),
        out_shape=jax.ShapeDtypeStruct((2, drafted, w.shape[1]), BF16),
        in_specs=[smem] + [vmem] * (2 * chips) + [pl.BlockSpec(memory_space=pl.ANY)],
        out_specs=vmem,
        scratch_shapes=[
            pltpu.VMEM((chips, depth, w.shape[1]), BF16),
            pltpu.SemaphoreType.DMA((chips,)),
        ],
        compiler_params=VMEM,
        name="project",
    )(seat, *mine, *theirs, w)


def vocab_kernel(seat_ref, *refs, pieces):
    hidden, (gain, w, out, normed, extra) = refs[:pieces], refs[pieces:]
    rows = normed.shape[0]

    @pl.when((pl.program_id(0) == 0) & (pl.program_id(1) == 0))
    def _():
        x = jnp.concatenate([ref[...].astype(F32) for ref in hidden], axis=0)
        normed[...] = (x * gain[...].astype(F32)).astype(BF16)
        squares = to_row(jnp.sum(x * x, axis=1, keepdims=True), eye_mask(rows))
        parts = jnp.concatenate(list(split3(squares)) + [jnp.zeros((13, LANES), F32)], axis=0)
        extra[...] = parts.astype(BF16)

    out[0, 0, :rows, :] = dot(normed[...], w[...]).astype(BF16)
    for n in range(0, out.shape[3], LANES):
        out[0, 0, rows:, n : n + LANES] = extra[...]


def vocab(seat, hidden, gain, w, chips):
    pieces = len(hidden)
    rows = pieces * hidden[0].shape[0]
    cols = w.shape[0]
    wide = w.shape[1] // (2 * chips)
    small = pl.BlockSpec(hidden[0].shape, lambda c, p, seat: (0, 0))
    return pl.pallas_call(
        functools.partial(vocab_kernel, pieces=pieces),
        out_shape=jax.ShapeDtypeStruct((2, chips, rows + 16, wide), BF16),
        grid_spec=pltpu.PrefetchScalarGridSpec(
            num_scalar_prefetch=1,
            grid=(2, chips),
            in_specs=[small] * pieces
            + [
                pl.BlockSpec((1, cols), lambda p, c, seat: (0, 0)),
                pl.BlockSpec((cols, wide), lambda p, c, seat: (0, 2 * c + (seat[0] + p + 1) % 2)),
            ],
            out_specs=pl.BlockSpec((1, 1, rows + 16, wide), lambda p, c, seat: (p, c, 0, 0)),
            scratch_shapes=[pltpu.VMEM((rows, cols), BF16), pltpu.VMEM((16, LANES), BF16)],
        ),
        compiler_params=VMEM,
        name="vocab",
    )(seat, *hidden, gain, w)


def row_sum(ref_value):
    return ref_value[0:1] + ref_value[1:2] + ref_value[2:3]


def pair_kernel(seat_ref, own, other, *outs, chips):
    chip = seat_ref[0] // 2
    rows = own.shape[1] - 16
    for k in range(chips):
        at = (chip + k) % chips
        both = own[at, :rows, :].astype(F32) + other[at, :rows, :].astype(F32)
        outs[k][:rows, :] = both.astype(BF16)
        squares = row_sum(own[at, rows:, :].astype(F32)) + row_sum(other[at, rows:, :].astype(F32))
        parts = list(split3(squares)) + [jnp.zeros((13, squares.shape[1]), F32)]
        outs[k][rows:, :] = jnp.concatenate(parts, axis=0).astype(BF16)


def pair(seat, own, other):
    chips = own.shape[0]
    smem = pl.BlockSpec(memory_space=pltpu.SMEM)
    vmem = pl.BlockSpec(memory_space=pltpu.VMEM)
    return pl.pallas_call(
        functools.partial(pair_kernel, chips=chips),
        out_shape=[jax.ShapeDtypeStruct(own.shape[1:], BF16)] * chips,
        in_specs=[smem, vmem, vmem],
        out_specs=[vmem] * chips,
        compiler_params=VMEM,
        name="pair",
    )(seat, own, other)


def close_kernel(place_ref, *refs, features):
    blocks, out, hold = refs[:-2], refs[-2], refs[-1]
    pieces, per, wide = out.shape
    rows = pieces * per
    acc, squares = None, None
    for ref in blocks:
        term = ref[:rows, :].astype(F32)
        part = row_sum(ref[rows:, :].astype(F32))
        acc = term if acc is None else acc + term
        squares = part if squares is None else squares + part
    column = to_column(squares[:, :LANES], eye_mask(rows))
    acc = acc * lax.rsqrt(column / features + EPSILON)
    for k in range(pieces):
        hold[k] = acc[k * per : (k + 1) * per]
    place = place_ref[0]
    for i in range(pieces):
        out[i] = hold[(place - i + pieces) % pieces].astype(BF16)


def close(place, blocks, pieces, features):
    rows, wide = blocks[0].shape
    per = (rows - 16) // pieces
    smem = pl.BlockSpec(memory_space=pltpu.SMEM)
    vmem = pl.BlockSpec(memory_space=pltpu.VMEM)
    return pl.pallas_call(
        functools.partial(close_kernel, features=features),
        out_shape=jax.ShapeDtypeStruct((pieces, per, wide), BF16),
        in_specs=[smem] + [vmem] * len(blocks),
        out_specs=vmem,
        scratch_shapes=[pltpu.VMEM((pieces, per, wide), F32)],
        compiler_params=VMEM,
        name="close",
    )(place, *blocks)


def per_device(
    latent_cache, draft_latent, query_nope, query_rope, parents, lengths, key_weight,
    value_weight, out_weight, residual, norm_gain, vocab_weight, *, seats, places,
):
    requests, cache_local, width = latent_cache.shape
    drafted, heads = query_nope.shape[1:3]
    draft_local = draft_latent.shape[1]
    features = residual.shape[2] * seats
    rows = requests * drafted
    chips = seats // 2
    per = heads // chips
    scaling = 1.0 / math.sqrt(query_nope.shape[3] + query_rope.shape[3])
    seat = lax.axis_index("seq")
    place = lax.axis_index("head")
    core = seat % 2
    seat1, place1 = seat.reshape(1), place.reshape(1)

    swap = [(i, i ^ 1) for i in range(seats)]

    def around(k):
        return [(i, ((i // 2 + k) % chips) * 2 + i % 2) for i in range(seats)]

    def turn(k):
        return [(i, (i + k) % places) for i in range(places)]

    qn = query_nope.reshape(rows * heads, -1)
    qr = query_rope.reshape(rows * heads, -1)
    offsets = jnp.arange(requests, dtype=jnp.int32)[:, None] * drafted
    link = jnp.where(parents >= 0, parents + offsets, -1).reshape(rows, 1)
    link = jnp.broadcast_to(link, (rows, rows))
    draft = draft_latent.transpose(0, 2, 1)
    draft = jnp.pad(draft, ((0, 0), (0, 0), (0, LANES - draft_local)))
    o, lse = attend(
        seat1, lengths, link, draft, qn, qr, key_weight, value_weight,
        latent_cache.transpose(0, 2, 1),
        drafted, draft_local, scaling,
    )

    other_o = lax.ppermute(lax.dynamic_index_in_dim(o, 1 - core, 0, keepdims=False), "seq", swap)
    other_lse = lax.ppermute(
        lax.dynamic_index_in_dim(lse, 1 - core, 0, keepdims=False), "seq", swap
    )
    blocks = join(seat1, o, lse, other_o, other_lse, chips)
    blocks = [blocks[0]] + [
        lax.ppermute(blocks[k], "seq", around(k)) for k in range(1, chips)
    ]
    own = combine(blocks, per, drafted)
    mine = [own] + [lax.ppermute(own, "seq", around(k)) for k in range(1, chips)]
    theirs = [lax.ppermute(x, "seq", swap) for x in mine]
    attention = project(seat1, mine, theirs, out_weight, per, drafted)

    share = rows // places
    attention = attention.reshape(rows, -1)
    parts = []
    for k in range(places):
        at = (place + k) % places
        part = lax.dynamic_slice_in_dim(attention, at * share, share, 0)
        parts.append(lax.ppermute(part, "head", turn(k)) if k else part)
    hidden = lax.dynamic_slice_in_dim(residual.reshape(rows, -1), place * share, share, 0)
    hidden = hidden.astype(F32) + sum(x.astype(F32) for x in parts)
    hidden = hidden.astype(BF16)
    hidden = [hidden] + [lax.ppermute(hidden, "head", turn(k)) for k in range(1, places)]
    sums = vocab(seat1, hidden, norm_gain.reshape(1, -1), vocab_weight, chips)
    other = lax.ppermute(sums[0], "seq", swap)
    blocks = pair(seat1, sums[1], other)
    blocks = [blocks[0]] + [
        lax.ppermute(blocks[k], "seq", around(k)) for k in range(1, chips)
    ]
    logits = close(place1, blocks, places, features)
    return logits.reshape(requests, drafted, -1)


def solution(mesh):
    in_specs = (
        P(None, "seq", None),
        P(None, "seq", None),
        P(None, None, "head", None),
        P(None, None, "head", None),
        P(),
        P(),
        P("head", None, None),
        P("head", None, None),
        P("head", "seq"),
        P(None, None, "seq"),
        P("seq"),
        P("seq", "head"),
    )
    out_specs = P(None, None, ("head", "seq"))
    body = functools.partial(per_device, seats=mesh.shape["seq"], places=mesh.shape["head"])
    return jax.shard_map(body, mesh=mesh, in_specs=in_specs, out_specs=out_specs, check_vma=False)
```

```python
import functools
import math

import jax
import jax.numpy as jnp
from jax import lax
from jax.experimental import pallas as pl
from jax.experimental.pallas import tpu as pltpu
from jax.sharding import PartitionSpec as P


NEGATIVE = -1e30
EPSILON = 1e-06
LANES = 128
F32 = jnp.float32
BF16 = jnp.bfloat16
ALONE = pltpu.CompilerParams(vmem_limit_bytes=60 * 1024 * 1024)
VMEM = pltpu.CompilerParams(vmem_limit_bytes=24 * 1024 * 1024)


def dot(a, b):
    return jnp.dot(a, b, preferred_element_type=F32)


def dot_t(a, b):
    return lax.dot_general(a, b, (((1,), (1,)), ((), ())), preferred_element_type=F32)


def eye_mask(rows):
    return lax.broadcasted_iota(jnp.int32, (rows, LANES), 0) == lax.broadcasted_iota(
        jnp.int32, (rows, LANES), 1
    )


def to_row(column, mask):
    return jnp.sum(jnp.where(mask, column, 0.0), axis=0, keepdims=True)


def to_column(row, mask):
    return jnp.sum(jnp.where(mask, row, 0.0), axis=1, keepdims=True)


def split3(x):
    hi = x.astype(BF16).astype(F32)
    mid = (x - hi).astype(BF16).astype(F32)
    lo = x - hi - mid
    return hi, mid, lo


def pad_rows(x, rows):
    if x.shape[0] == rows:
        return x
    return jnp.concatenate([x, jnp.zeros((rows - x.shape[0], x.shape[1]), x.dtype)], axis=0)


def attend_kernel(*refs, second, group, heads, drafted, draft_local, chips, scaling):
    if second:
        (seat_ref, len_ref, parent_ref, draft_ref, o1_ref, lse1_ref), refs = refs[:6], refs[6:]
    else:
        (seat_ref, len_ref), refs = refs[:2], refs[2:]
    (qn_hbm, qr_hbm, kw_hbm, vw_hbm, cache_hbm), refs = refs[:5], refs[5:]
    outs, refs = (refs[:chips], refs[chips:]) if second else (refs[:2], refs[2:])
    qn, qr, qnf, qrf, kw, vw, keys, q0, q1, s0, s1, p0, p1, sems = refs[:14]
    if second:
        tree, pay, lses = refs[14:]
    else:
        lses = outs[1]
    _, width, cache_local = cache_hbm.shape
    latent, value = vw_hbm.shape[1:]
    rows = drafted * heads
    per = heads // chips
    steps = heads // group
    q_refs, s_refs, p_refs = (q0, q1), (s0, s1), (p0, p1)
    chunk = 256
    cuts = 4
    cut = cache_local // cuts
    total_keys = cache_local + (LANES if second else 0)
    seat = seat_ref[0]
    core, chip = seat % 2, seat // 2
    held = seat + 1 - 2 * core if second else seat
    scale2 = scaling * math.log2(math.e)

    def heads_of(src, dst, k, sem):
        at = pl.ds((chip + k) % chips * per, per)
        return pltpu.make_async_copy(src.at[at], dst.at[pl.ds(k * per, per)], sem)

    def keys_of(n):
        src = cache_hbm.at[core, :, pl.ds(n * cut, cut)]
        return pltpu.make_async_copy(src, keys.at[:, pl.ds(n * cut, cut)], sems.at[2 + n])

    own_rows = pl.ds(pl.multiple_of(core * rows, rows), rows)
    q_copies = [
        pltpu.make_async_copy(qn_hbm.at[own_rows], qn, sems.at[0]),
        pltpu.make_async_copy(qr_hbm.at[own_rows], qr, sems.at[1]),
    ]
    key_copies = [keys_of(n) for n in range(cuts)]
    base = 2 + cuts
    kw_copies = [heads_of(kw_hbm, kw, k, sems.at[base + k]) for k in range(chips)]
    vw_copies = [heads_of(vw_hbm, vw, k, sems.at[base + chips + k]) for k in range(chips)]
    for copy in q_copies + kw_copies[:1] + key_copies + kw_copies[1:] + vw_copies:
        copy.start()

    mask = eye_mask(drafted)
    if second:
        parent = parent_ref[pl.ds(core, 1), :].astype(F32)
        lane = lax.broadcasted_iota(jnp.int32, (drafted, drafted), 1)
        sub = lax.broadcasted_iota(jnp.int32, (drafted, drafted), 0)
        column = jnp.sum(jnp.where(lane == sub, parent, 0.0), axis=1, keepdims=True)
        linked = (column == lane.astype(F32)) | (lane == sub)
        reach = jnp.where(linked, 1.0, 0.0).astype(BF16)
        for _ in range(max(1, (drafted - 1).bit_length())):
            reach = jnp.where(dot(reach, reach) > 0.5, 1.0, 0.0).astype(BF16)
        lane = lax.broadcasted_iota(jnp.int32, (drafted, LANES), 1)
        sub = lax.broadcasted_iota(jnp.int32, (drafted, LANES), 0)
        pick = ((sub == seat * draft_local + lane) & (lane < draft_local)) | (
            (sub == held * draft_local + lane - draft_local)
            & (lane >= draft_local)
            & (lane < 2 * draft_local)
        )
        tree[...] = dot(reach, jnp.where(pick, 1.0, 0.0).astype(BF16))
        keys[:, cache_local:] = draft_ref[...]

    live = len_ref[core] - held * cache_local

    def absorb(slot, g):
        for i in range(group):
            r = g * group + i
            at = pl.ds((chip + r // per) % chips * per + r % per, drafted, stride=heads)
            to = slice(i * drafted, (i + 1) * drafted)
            q_refs[slot][to, :latent] = dot(qnf[at, :].astype(BF16), kw[r]).astype(BF16)
            q_refs[slot][to, latent:] = qrf[at, :].astype(BF16)

    def score_pieces(slot):
        q_ref, s_ref = q_refs[slot], s_refs[slot]

        def cached(n):
            s = dot(q_ref[...], keys[:, n : n + chunk])
            at = lax.broadcasted_iota(jnp.int32, (1, chunk), 1) + n
            s_ref[:, n : n + chunk] = s * scale2 + jnp.where(at < live, 0.0, NEGATIVE)

        def drafts():
            s = dot(q_ref[...], keys[:, cache_local:])[:, :LANES]
            for i in range(group):
                at = slice(i * drafted, (i + 1) * drafted)
                s_ref[at, cache_local:] = jnp.where(tree[...] > 0.5, s[at] * scale2, NEGATIVE)

        pieces = [functools.partial(cached, n) for n in range(0, cache_local, chunk)]
        return pieces + ([drafts] if second else [])

    def soft_pieces(slot, stats):
        s_ref, p_ref = s_refs[slot], p_refs[slot]

        def piece(i):
            at = slice(i * drafted, (i + 1) * drafted)
            top = s_ref[at, 0:LANES]
            for n in range(LANES, total_keys, LANES):
                top = jnp.maximum(top, s_ref[at, n : n + LANES])
            top = jnp.max(top, axis=1, keepdims=True)
            total = None
            for n in range(0, total_keys, LANES):
                p = jnp.exp2(s_ref[at, n : n + LANES] - top)
                p_ref[at, n : n + LANES] = p.astype(BF16)
                total = p if total is None else total + p
            total = jnp.sum(total, axis=1, keepdims=True)
            stats.append((total, top + jnp.log2(total)))

        return [functools.partial(piece, i) for i in range(group)]

    def store(r, o, lse):
        if second:
            before = to_column(lse1_ref[pl.ds(r, 1), :], mask)
            top = jnp.maximum(before, lse)
            wa, wb = jnp.exp2(before - top), jnp.exp2(lse - top)
            total = wa + wb
            o = o1_ref[r].astype(F32) * (wa / total) + o * (wb / total)
            lse = top + jnp.log2(total)
            at = pl.ds(pl.multiple_of(r % per * drafted, drafted), drafted)
            pay[r // per, at, :] = o.astype(BF16)
        else:
            outs[0][r] = o.astype(BF16)
        lses[pl.ds(r, 1), :] = to_row(lse, mask)

    def finish(slot, g, stats):
        mixed = dot_t(p_refs[slot][...], keys[:latent, :total_keys])
        pairs = 2 if group % 2 == 0 else 1
        for i in range(0, group, pairs):
            r = g * group + i
            parts, weights = [], []
            for j in range(pairs):
                m = mixed[(i + j) * drafted : (i + j + 1) * drafted]
                parts.append((m * (1.0 / stats[i + j][0])).astype(BF16))
                weights.append(vw[r + j])
            if pairs == 1:
                store(r, dot(parts[0], weights[0]), stats[i][1])
                continue
            both = dot(jnp.concatenate(parts, axis=0), jnp.concatenate(weights, axis=1))
            for j in range(pairs):
                o = both[j * drafted : (j + 1) * drafted, j * value : (j + 1) * value]
                store(r + j, o, stats[i + j][1])

    def interleave(slot_next, slot, g):
        stats = []
        first = score_pieces(slot_next) if slot_next is not None else []
        second_list = soft_pieces(slot, stats)
        count = max(len(first), len(second_list))
        done = 0
        for j in range(count):
            if j < len(first):
                first[j]()
            while done < len(second_list) and done * max(len(first), 1) <= j * len(second_list):
                second_list[done]()
                done += 1
        while done < len(second_list):
            second_list[done]()
            done += 1
        finish(slot, g, stats)

    lazy = group == per or 2 * group == per

    def await_heads(src, dst, first, g, odd):
        if lazy and (group == per or not odd):
            k = g * group // per
            heads_of(src, dst, k, sems.at[first + k]).wait()

    def await_kw(g, odd):
        await_heads(kw_hbm, kw, base, g, odd)

    def await_vw(g, odd):
        await_heads(vw_hbm, vw, base + chips, g, odd)

    q_copies[0].wait()
    qnf[...] = qn[...].astype(F32)
    q_copies[1].wait()
    qrf[...] = qr[...].astype(F32)
    if lazy:
        await_kw(0, False)
    else:
        for copy in kw_copies:
            copy.wait()
    absorb(0, 0)
    pieces = score_pieces(0)
    for n, piece in enumerate(pieces):
        if n * chunk % cut == 0 and n * chunk < cache_local:
            key_copies[n * chunk // cut].wait()
        piece()
    for copy in [] if lazy else vw_copies:
        copy.wait()

    def step(i, carry):
        g = 2 * i
        await_kw(g + 1, True)
        await_kw(g + 2, False)
        await_vw(g, False)
        await_vw(g + 1, True)
        absorb(1, g + 1)
        interleave(1, 0, g)
        absorb(0, g + 2)
        interleave(0, 1, g + 1)
        return carry

    if steps > 2:
        lax.fori_loop(0, steps // 2 - 1, step, 0)
    await_kw(steps - 1, True)
    await_vw(steps - 2, False)
    await_vw(steps - 1, True)
    absorb(1, steps - 1)
    interleave(1, 0, steps - 2)
    interleave(None, 1, steps - 1)

    if second:
        done = []
        tail = max(8, per)
        for k in range(chips):
            lse = pad_rows(lses[k * per : (k + 1) * per, :], tail)
            hi, mid, lo = split3(lse)
            extra = jnp.concatenate([hi, mid, lo, jnp.zeros_like(lo)], axis=0)
            pay[k, per * drafted :, :] = extra.astype(BF16)
            done.append(pltpu.make_async_copy(pay.at[k], outs[k], sems.at[k]))
            done[-1].start()
        for copy in done:
            copy.wait()


def attend(seat, lengths, extras, qn, qr, kw, vw, cache, drafted, draft_local, chips, scaling):
    _, width, cache_local = cache.shape
    heads, _, value = vw.shape
    second = len(extras) > 0
    group = min(8, heads // 2)
    per = heads // chips
    block = group * drafted
    rows = drafted * heads
    keys = cache_local + (LANES if second else 0)
    hbm = pl.BlockSpec(memory_space=pltpu.HBM)
    smem = pl.BlockSpec(memory_space=pltpu.SMEM)
    vmem = pl.BlockSpec(memory_space=pltpu.VMEM)
    free = pl.BlockSpec(memory_space=pl.ANY)
    if second:
        payload = (per * drafted + 4 * max(8, per), value)
        out_shape = [jax.ShapeDtypeStruct(payload, BF16)] * chips
        out_specs = [free] * chips
    else:
        out_shape = [
            jax.ShapeDtypeStruct((heads, drafted, value), BF16),
            jax.ShapeDtypeStruct((heads, LANES), F32),
        ]
        out_specs = [vmem, vmem]
    scratch = [
        pltpu.VMEM((rows, qn.shape[1]), BF16),
        pltpu.VMEM((rows, qr.shape[1]), BF16),
        pltpu.VMEM((rows, qn.shape[1]), F32),
        pltpu.VMEM((rows, qr.shape[1]), F32),
        pltpu.VMEM(kw.shape, BF16),
        pltpu.VMEM(vw.shape, BF16),
        pltpu.VMEM((width, cache_local + (2 * LANES if second else 0)), BF16),
        pltpu.VMEM((block, width), BF16),
        pltpu.VMEM((block, width), BF16),
        pltpu.VMEM((block, keys), F32),
        pltpu.VMEM((block, keys), F32),
        pltpu.VMEM((block, keys), BF16),
        pltpu.VMEM((block, keys), BF16),
        pltpu.SemaphoreType.DMA((6 + 2 * chips,)),
    ]
    if second:
        scratch += [
            pltpu.VMEM((drafted, LANES), F32),
            pltpu.VMEM((chips,) + payload, BF16),
            pltpu.VMEM((heads, LANES), F32),
        ]
    return pl.pallas_call(
        functools.partial(
            attend_kernel, second=second, group=group, heads=heads, drafted=drafted,
            draft_local=draft_local, chips=chips, scaling=scaling,
        ),
        out_shape=out_shape,
        in_specs=[smem, smem] + [vmem] * len(extras) + [hbm] * 5,
        out_specs=out_specs,
        scratch_shapes=scratch,
        compiler_params=ALONE,
        name="attend_second" if second else "attend_first",
    )(seat, lengths, *extras, qn, qr, kw, vw, cache)


def combine_kernel(*refs, per, drafted):
    blocks, out = refs[:-1], refs[-1]
    mask = eye_mask(drafted)
    tail = max(8, per)
    base = per * drafted
    lses = []
    for ref in blocks:
        extra = ref[base:, :].astype(F32)
        lses.append(extra[:tail] + extra[tail : 2 * tail] + extra[2 * tail : 3 * tail])
    top = functools.reduce(jnp.maximum, lses)
    weights = [jnp.exp2(x - top) for x in lses]
    total = functools.reduce(jnp.add, weights)
    weights = [w / total for w in weights]
    for j in range(per):
        at = slice(j * drafted, (j + 1) * drafted)
        acc = None
        for ref, w in zip(blocks, weights):
            term = ref[at, :].astype(F32) * to_column(w[j : j + 1], mask)
            acc = term if acc is None else acc + term
        out[at, :] = acc.astype(BF16)


def combine(blocks, per, drafted):
    vmem = pl.BlockSpec(memory_space=pltpu.VMEM)
    return pl.pallas_call(
        functools.partial(combine_kernel, per=per, drafted=drafted),
        out_shape=jax.ShapeDtypeStruct((per * drafted, blocks[0].shape[1]), BF16),
        in_specs=[vmem] * len(blocks),
        out_specs=vmem,
        compiler_params=VMEM,
        name="combine",
    )(*blocks)


def fetch_kernel(after_ref, src, out, sem):
    copy = pltpu.make_async_copy(src, out, sem)
    copy.start()
    copy.wait()


def fetch(after, w):
    return pl.pallas_call(
        fetch_kernel,
        out_shape=jax.ShapeDtypeStruct(w.shape, w.dtype),
        in_specs=[
            pl.BlockSpec(memory_space=pl.ANY),
            pl.BlockSpec(memory_space=pltpu.HBM),
        ],
        out_specs=pl.BlockSpec(memory_space=pltpu.VMEM),
        scratch_shapes=[pltpu.SemaphoreType.DMA(())],
        cost_estimate=pl.CostEstimate(
            flops=1 << 31, transcendentals=0, bytes_accessed=2 * w.size
        ),
        compiler_params=pltpu.CompilerParams(vmem_limit_bytes=48 * 1024 * 1024),
        name="fetch",
    )(after, w)


def project_kernel(seat_ref, place_ref, *refs, chips, per, drafted, places):
    mine, theirs = refs[:chips], refs[chips : 2 * chips]
    w_hbm, refs = refs[2 * chips], refs[2 * chips + 1 :]
    outs, (w, hold, sems, w_sems) = refs[:places], refs[places:]
    seat, place = seat_ref[0], place_ref[0]
    core, chip = seat % 2, seat // 2
    depth = w.shape[1]
    loads = []
    for k in range(chips):
        at = pl.ds(pl.multiple_of((chip - k + chips) % chips * depth, depth), depth)
        loads.append(pltpu.make_async_copy(w_hbm.at[at], w.at[k], w_sems.at[k]))
        loads[-1].start()
    share = hold.shape[1]
    acc = None
    for k in range(chips):
        sides = []
        for side in (mine[k], theirs[k]):
            parts = [side[j * drafted : (j + 1) * drafted, :] for j in range(per)]
            sides.append(jnp.concatenate(parts, axis=1) if per > 1 else parts[0])
        x = jnp.concatenate(sides, axis=0)
        loads[k].wait()
        term = dot(x, w[k])
        acc = term if acc is None else acc + term
    blocks = drafted // share
    for i in range(2 * blocks):
        at = core * blocks + i if i < blocks else (1 - core) * blocks + i - blocks
        hold[at] = acc[i * share : (i + 1) * share].astype(BF16)
    copies = []
    for k in range(places):
        copies.append(
            pltpu.make_async_copy(hold.at[(place + k) % places], outs[k], sems.at[k])
        )
        copies[-1].start()
    for copy in copies:
        copy.wait()


def project(seat, place, mine, theirs, w, per, drafted, places):
    chips = len(mine)
    share = 2 * drafted // places
    smem = pl.BlockSpec(memory_space=pltpu.SMEM)
    vmem = pl.BlockSpec(memory_space=pltpu.VMEM)
    return pl.pallas_call(
        functools.partial(
            project_kernel, chips=chips, per=per, drafted=drafted, places=places
        ),
        out_shape=[jax.ShapeDtypeStruct((share, w.shape[1]), BF16)] * places,
        in_specs=[smem, smem] + [vmem] * (2 * chips) + [pl.BlockSpec(memory_space=pltpu.HBM)],
        out_specs=[pl.BlockSpec(memory_space=pl.ANY)] * places,
        scratch_shapes=[
            pltpu.VMEM((chips, w.shape[0] // chips, w.shape[1]), BF16),
            pltpu.VMEM((places, share, w.shape[1]), BF16),
            pltpu.SemaphoreType.DMA((places,)),
            pltpu.SemaphoreType.DMA((chips,)),
        ],
        compiler_params=pltpu.CompilerParams(vmem_limit_bytes=58 * 1024 * 1024),
        name="project",
    )(seat, place, *mine, *theirs, w)


def vocab_kernel(seat_ref, *refs, pieces, chips):
    hidden, (gain, w, own, other, hold, sems) = refs[:pieces], refs[pieces:]
    core = seat_ref[0] % 2
    wide = hold.shape[3]
    rows = hold.shape[2] - 16
    x = jnp.concatenate([ref[...].astype(F32) for ref in hidden], axis=0)
    normed = (x * gain[...].astype(F32)).astype(BF16)
    squares = to_row(jnp.sum(x * x, axis=1, keepdims=True), eye_mask(rows))
    parts = jnp.concatenate(list(split3(squares)) + [jnp.zeros((13, LANES), F32)], axis=0)
    extra = jnp.concatenate([parts.astype(BF16)] * (wide // LANES), axis=1)
    for c in range(chips):
        for p in range(2):
            to = (core + p) % 2
            n = (2 * c + p) * wide
            hold[to, c, :rows, :] = dot(normed, w[:, n : n + wide]).astype(BF16)
            hold[to, c, rows:, :] = extra
    copies = [
        pltpu.make_async_copy(hold.at[1], other, sems.at[1]),
        pltpu.make_async_copy(hold.at[0], own, sems.at[0]),
    ]
    for copy in copies:
        copy.start()
    for copy in copies:
        copy.wait()


def vocab(seat, hidden, gain, w, chips):
    pieces = len(hidden)
    rows = pieces * hidden[0].shape[0]
    wide = w.shape[1] // (2 * chips)
    smem = pl.BlockSpec(memory_space=pltpu.SMEM)
    vmem = pl.BlockSpec(memory_space=pltpu.VMEM)
    shape = (chips, rows + 16, wide)
    return pl.pallas_call(
        functools.partial(vocab_kernel, pieces=pieces, chips=chips),
        out_shape=[jax.ShapeDtypeStruct(shape, BF16)] * 2,
        in_specs=[smem] + [vmem] * (pieces + 2),
        out_specs=[pl.BlockSpec(memory_space=pl.ANY)] * 2,
        scratch_shapes=[pltpu.VMEM((2,) + shape, BF16), pltpu.SemaphoreType.DMA((2,))],
        compiler_params=VMEM,
        name="vocab",
    )(seat, *hidden, gain, w)


def row_sum(ref_value):
    return ref_value[0:1] + ref_value[1:2] + ref_value[2:3]


def pair_kernel(seat_ref, own, other, *outs, chips):
    chip = seat_ref[0] // 2
    rows = own.shape[1] - 16
    for k in range(chips):
        at = (chip + k) % chips
        both = own[at, :rows, :].astype(F32) + other[at, :rows, :].astype(F32)
        outs[k][:rows, :] = both.astype(BF16)
        squares = row_sum(own[at, rows:, :].astype(F32)) + row_sum(other[at, rows:, :].astype(F32))
        parts = list(split3(squares)) + [jnp.zeros((13, squares.shape[1]), F32)]
        outs[k][rows:, :] = jnp.concatenate(parts, axis=0).astype(BF16)


def pair(seat, own, other):
    chips = own.shape[0]
    smem = pl.BlockSpec(memory_space=pltpu.SMEM)
    vmem = pl.BlockSpec(memory_space=pltpu.VMEM)
    return pl.pallas_call(
        functools.partial(pair_kernel, chips=chips),
        out_shape=[jax.ShapeDtypeStruct(own.shape[1:], BF16)] * chips,
        in_specs=[smem, vmem, vmem],
        out_specs=[vmem] * chips,
        compiler_params=VMEM,
        name="pair",
    )(seat, own, other)


def close_kernel(place_ref, *refs, features):
    blocks, out, hold = refs[:-2], refs[-2], refs[-1]
    pieces, per, wide = out.shape
    rows = pieces * per
    acc, squares = None, None
    for ref in blocks:
        term = ref[:rows, :].astype(F32)
        part = row_sum(ref[rows:, :].astype(F32))
        acc = term if acc is None else acc + term
        squares = part if squares is None else squares + part
    column = to_column(squares[:, :LANES], eye_mask(rows))
    acc = acc * lax.rsqrt(column / features + EPSILON)
    for k in range(pieces):
        hold[k] = acc[k * per : (k + 1) * per]
    place = place_ref[0]
    for i in range(pieces):
        out[i] = hold[(place - i + pieces) % pieces].astype(BF16)


def close(place, blocks, pieces, features):
    rows, wide = blocks[0].shape
    per = (rows - 16) // pieces
    smem = pl.BlockSpec(memory_space=pltpu.SMEM)
    vmem = pl.BlockSpec(memory_space=pltpu.VMEM)
    return pl.pallas_call(
        functools.partial(close_kernel, features=features),
        out_shape=jax.ShapeDtypeStruct((pieces, per, wide), BF16),
        in_specs=[smem] + [vmem] * len(blocks),
        out_specs=vmem,
        scratch_shapes=[pltpu.VMEM((pieces, per, wide), F32)],
        compiler_params=VMEM,
        name="close",
    )(place, *blocks)


def per_device(
    latent_cache, draft_latent, query_nope, query_rope, parents, lengths, key_weight,
    value_weight, out_weight, residual, norm_gain, vocab_weight, *, seats, places,
):
    requests, cache_local, width = latent_cache.shape
    drafted, heads = query_nope.shape[1:3]
    draft_local = draft_latent.shape[1]
    features = residual.shape[2] * seats
    rows = requests * drafted
    chips = seats // 2
    per = heads // chips
    scaling = 1.0 / math.sqrt(query_nope.shape[3] + query_rope.shape[3])
    seat = lax.axis_index("seq")
    place = lax.axis_index("head")
    core = seat % 2
    seat1, place1 = seat.reshape(1), place.reshape(1)

    swap = [(i, i ^ 1) for i in range(seats)]

    def around(k):
        return [(i, ((i // 2 + k) % chips) * 2 + i % 2) for i in range(seats)]

    def turn(k):
        return [(i, (i + k) % places) for i in range(places)]

    qn = query_nope.reshape(rows * heads, -1)
    qr = query_rope.reshape(rows * heads, -1)
    cache = latent_cache.transpose(0, 2, 1)
    other_cache = lax.ppermute(cache, "seq", swap)
    other_draft = lax.ppermute(draft_latent, "seq", swap)
    sizes = (drafted, draft_local, chips, scaling)
    o, lse = attend(seat1, lengths, (), qn, qr, key_weight, value_weight, cache, *sizes)
    draft = jnp.concatenate([draft_latent, other_draft], axis=1)
    draft = lax.dynamic_index_in_dim(draft, core, 0, keepdims=False).T
    draft = jnp.pad(draft, ((0, 0), (0, 2 * LANES - draft.shape[1])))
    other_cache, o, lse = lax.optimization_barrier((other_cache, o, lse))
    blocks = attend(
        seat1, lengths, (parents, draft, o, lse), qn, qr, key_weight, value_weight, other_cache,
        *sizes,
    )
    blocks = [blocks[0]] + [
        lax.ppermute(blocks[k], "seq", around(k)) for k in range(1, chips)
    ]
    own = combine(blocks, per, drafted)
    mine = [own] + [lax.ppermute(own, "seq", around(k)) for k in range(1, chips)]
    theirs = [lax.ppermute(x, "seq", swap) for x in mine]
    parts = project(
        seat1, place1, mine, theirs, out_weight, per, drafted, places
    )
    share = rows // places
    parts = [parts[0]] + [lax.ppermute(parts[k], "head", turn(k)) for k in range(1, places)]
    hidden = lax.dynamic_slice_in_dim(residual.reshape(rows, -1), place * share, share, 0)
    hidden = hidden.astype(F32) + sum(x.astype(F32) for x in parts)
    hidden = hidden.astype(BF16)
    vocab_weight = fetch(hidden, vocab_weight)
    hidden = [hidden] + [lax.ppermute(hidden, "head", turn(k)) for k in range(1, places)]
    own, other = vocab(seat1, hidden, norm_gain.reshape(1, -1), vocab_weight, chips)
    blocks = pair(seat1, own, lax.ppermute(other, "seq", swap))
    blocks = [blocks[0]] + [
        lax.ppermute(blocks[k], "seq", around(k)) for k in range(1, chips)
    ]
    logits = close(place1, blocks, places, features)
    return logits.reshape(requests, drafted, -1)


def solution(mesh):
    in_specs = (
        P(None, "seq", None),
        P(None, "seq", None),
        P(None, None, "head", None),
        P(None, None, "head", None),
        P(),
        P(),
        P("head", None, None),
        P("head", None, None),
        P("head", "seq"),
        P(None, None, "seq"),
        P("seq"),
        P("seq", "head"),
    )
    out_specs = P(None, None, ("head", "seq"))
    body = functools.partial(per_device, seats=mesh.shape["seq"], places=mesh.shape["head"])
    return jax.shard_map(body, mesh=mesh, in_specs=in_specs, out_specs=out_specs, check_vma=False)
```
